8 devices in a mesh: tp: 2 (over z, y), dp: 2 (over x), pp: 2 (over core).
Axes of the slice: x: 2, y: 2, z: 1, core: 2. Of those that a mesh axis runs over, the one named last changes fastest.
Arguments:
- master: float32 [32000, 1152], P('tp')
- exp_avg: float32 [32000, 1152], P('tp')
- exp_avg_sq: float32 [32000, 1152], P('tp')
- stage_ids: int32 [2, 12, 768], P('pp', 'dp')
- stage_acts: bfloat16 [2, 12, 768, 1152], P('pp', 'dp')
Outputs:
- output 1: float32 [32000, 1152], P('tp')
- output 2: float32 [32000, 1152], P('tp')
- output 3: float32 [32000, 1152], P('tp')
- output 4: bfloat16 [32000, 1152], P('tp')
All inputs are finite; a program needn't handle non-finite values.
Results may differ from the reference program's by a relative error of at most 0.001.
Values sent between devices are 32-bit elements.
A program may use at most 2 GiB of HBM per device.

```python
import math
import jax
import jax.numpy as jnp
from jax import lax

VOCAB_SIZE = 32000
MODEL_DIM = 1152
SEQ_LEN = 768
BATCH_DEV = 6
DATA_REPL = 2
PIPE_STAGES = 2
OPT_STEP = 10
TOKEN_BLOCK = 128

BATCH_ALL = BATCH_DEV * DATA_REPL
TOKENS_REPL = BATCH_DEV * SEQ_LEN
LOG_SPAN = math.ceil(math.log2(VOCAB_SIZE))
LEARN_RATE = 0.003
BETA_ONE = 0.9
BETA_TWO = 0.95
ADAM_EPS = 1e-8
WEIGHT_DECAY = 0.1
CLIP_NORM = 1.0


def draw_ids(key, perm):
    key_exp, key_rank = jax.random.split(key)
    ids_shape = (PIPE_STAGES, BATCH_ALL, SEQ_LEN)
    exponents = jax.random.randint(key_exp, ids_shape, 0, LOG_SPAN + 1)
    upper_bound = jnp.minimum(jnp.left_shift(jnp.int32(1), exponents), VOCAB_SIZE)
    ranks = jax.random.randint(key_rank, ids_shape, 0, upper_bound)
    tokens = perm[ranks]
    tokens = tokens.at[:, 0, 0].set(0)
    tokens = tokens.at[:, BATCH_ALL - 1, SEQ_LEN - 1].set(VOCAB_SIZE - 1)
    return tokens.astype(jnp.int32)


def setup_inputs(seed: int = 0) -> dict:
    key = jax.random.key(seed)
    k_tab, k_avg, k_sq, k_perm, k_ids, k_act, k_hid = jax.random.split(key, 7)
    table_shape = (VOCAB_SIZE, MODEL_DIM)
    elem_scale = (VOCAB_SIZE * MODEL_DIM) ** -0.5
    master = jax.random.normal(k_tab, table_shape, jnp.float32) * MODEL_DIM ** -0.5
    exp_avg = jax.random.normal(k_avg, table_shape, jnp.float32) * (0.3 * elem_scale)
    exp_avg_sq = jnp.exp(0.5 * jax.random.normal(k_sq, table_shape, jnp.float32)) * (0.09 * elem_scale * elem_scale)
    perm = jax.random.permutation(k_perm, VOCAB_SIZE)
    stage_ids = draw_ids(k_ids, perm)
    grad_scale = 0.08 * math.sqrt(DATA_REPL / TOKENS_REPL)
    stage_acts = jax.random.normal(k_act, (PIPE_STAGES, BATCH_ALL, SEQ_LEN, MODEL_DIM), jnp.float32) * grad_scale
    label_pull = math.log(VOCAB_SIZE) / math.sqrt(MODEL_DIM)
    noise = jax.random.normal(k_hid, (BATCH_ALL, SEQ_LEN, MODEL_DIM), jnp.float32)
    hidden = math.sqrt(1.0 - label_pull * label_pull) * noise + (label_pull * math.sqrt(MODEL_DIM)) * master[stage_ids[PIPE_STAGES - 1]]
    stage_acts = stage_acts.at[PIPE_STAGES - 1].set(hidden)
    return {"master": master, "exp_avg": exp_avg, "exp_avg_sq": exp_avg_sq, "stage_ids": stage_ids, "stage_acts": stage_acts.astype(jnp.bfloat16)}


def head_block(table_bf, hid_block, lab_block):
    logits = jnp.dot(hid_block, table_bf.T, preferred_element_type=jnp.float32)
    prob_mat = jax.nn.softmax(logits, axis=-1)
    is_label = lab_block[:, None] == jnp.arange(VOCAB_SIZE, dtype=jnp.int32)[None, :]
    dlogits = (jnp.where(is_label, prob_mat - 1.0, prob_mat) / TOKENS_REPL).astype(jnp.bfloat16)
    return jnp.dot(dlogits.T, hid_block, preferred_element_type=jnp.float32)


def replica_grad(table_bf, ids_in, dx_in, hidden, labels):
    grad_embed = jax.ops.segment_sum(dx_in.astype(jnp.float32), ids_in, num_segments=VOCAB_SIZE)

    def add_block(acc_grad, block_in):
        return acc_grad + head_block(table_bf, block_in[0], block_in[1]), None

    hid_blocks = hidden.reshape(-1, TOKEN_BLOCK, MODEL_DIM)
    lab_blocks = labels.reshape(-1, TOKEN_BLOCK)
    return lax.scan(add_block, grad_embed, (hid_blocks, lab_blocks))[0]


def reference(master, exp_avg, exp_avg_sq, stage_ids, stage_acts):
    table_bf = master.astype(jnp.bfloat16)
    ids_in = stage_ids[0].reshape(DATA_REPL, TOKENS_REPL)
    labels = stage_ids[PIPE_STAGES - 1].reshape(DATA_REPL, TOKENS_REPL)
    dx_in = stage_acts[0].reshape(DATA_REPL, TOKENS_REPL, MODEL_DIM)
    hidden = stage_acts[PIPE_STAGES - 1].reshape(DATA_REPL, TOKENS_REPL, MODEL_DIM)

    def add_replica(acc_grad, block_in):
        return acc_grad + replica_grad(table_bf, block_in[0], block_in[1], block_in[2], block_in[3]), None

    zero_grad = jnp.zeros((VOCAB_SIZE, MODEL_DIM), jnp.float32)
    grad_sum = lax.scan(add_replica, zero_grad, (ids_in, dx_in, hidden, labels))[0]
    gradient = grad_sum / DATA_REPL
    norm_val = jnp.sqrt(jnp.sum(gradient * gradient))
    gradient = gradient * (CLIP_NORM / jnp.maximum(norm_val, CLIP_NORM))
    new_avg = BETA_ONE * exp_avg + (1.0 - BETA_ONE) * gradient
    new_avg_sq = BETA_TWO * exp_avg_sq + (1.0 - BETA_TWO) * gradient * gradient
    corr_one = 1.0 - BETA_ONE ** OPT_STEP
    corr_two = 1.0 - BETA_TWO ** OPT_STEP
    step_dir = (new_avg / corr_one) / (jnp.sqrt(new_avg_sq / corr_two) + ADAM_EPS)
    new_master = master - LEARN_RATE * (step_dir + WEIGHT_DECAY * master)
    return new_master, new_avg, new_avg_sq, new_master.astype(jnp.bfloat16)
```

```python
import functools

import jax
import jax.numpy as jnp
from jax import lax
from jax.experimental import pallas as pl
from jax.experimental.pallas import tpu as pltpu
from jax.sharding import PartitionSpec as P

LEARN_RATE = 0.003
BETA_ONE = 0.9
BETA_TWO = 0.95
ADAM_EPS = 1e-8
WEIGHT_DECAY = 0.1
CLIP_NORM = 1.0
OPT_STEP = 10
VMEM_CAP = 63 * 1024 * 1024
F32 = jnp.float32
BF16 = jnp.bfloat16
AXES = ("tp", "dp", "pp")
ANY = pl.ANY


def params(n_axes=1):
    return pltpu.CompilerParams(dimension_semantics=("arbitrary",) * n_axes, vmem_limit_bytes=VMEM_CAP)


def logits_kernel(n_sub, stage_ref, fa_ref, fb_ref, e_ref, *rest):
    lg_ref, f_ref, m_ref, z_ref = rest[-4:]

    @pl.when(pl.program_id(0) == 0)
    def _():
        @pl.when(stage_ref[0] == 1)
        def _():
            f_ref[...] = fa_ref[...].astype(BF16)

        @pl.when(stage_ref[0] == 0)
        def _():
            f_ref[...] = fb_ref[...].astype(BF16)

        m_ref[...] = jnp.full_like(m_ref, -jnp.inf)
        z_ref[...] = jnp.zeros_like(z_ref)

    width = f_ref.shape[0] // n_sub
    for j in range(n_sub):
        cols = slice(j * width, (j + 1) * width)
        lg_ref[:, cols] = lax.dot_general(e_ref[...], f_ref[cols, :], (((1,), (1,)), ((), ())), preferred_element_type=F32)
        m_old = m_ref[:, cols]
        m_new = jnp.maximum(m_old, jnp.max(lg_ref[:, cols], axis=0, keepdims=True))
        part = jnp.sum(jnp.exp(lg_ref[:, cols] - m_new), axis=0, keepdims=True)
        z_ref[:, cols] = z_ref[:, cols] * jnp.exp(m_old - m_new) + part
        m_ref[:, cols] = m_new


def logits_call(stage, fa, fa_blk, fb, fb_blk, e_bf, t_blk, tb, vb, tok_all, prev):
    vq, d = e_bf.shape
    first = prev is None
    in_specs = [
        pl.BlockSpec((tb, d), lambda v, s: (fa_blk, 0)),
        pl.BlockSpec((tb, d), lambda v, s: (fb_blk, 0)),
        pl.BlockSpec((vb, d), lambda v, s: (v, 0)),
    ] + ([] if first else [pl.BlockSpec(memory_space=ANY)] * 2)
    out_specs = [
        pl.BlockSpec((vb, tb), lambda v, s: (v, t_blk)),
        pl.BlockSpec((tb, d), lambda v, s: (t_blk, 0)),
        pl.BlockSpec((1, tb), lambda v, s: (0, 0)),
        pl.BlockSpec((1, tb), lambda v, s: (0, 0)),
    ]
    n_sub = max(1, tb // 256)
    return pl.pallas_call(
        functools.partial(logits_kernel, n_sub),
        grid_spec=pltpu.PrefetchScalarGridSpec(num_scalar_prefetch=1, grid=(vq // vb,), in_specs=in_specs, out_specs=out_specs),
        out_shape=[
            jax.ShapeDtypeStruct((vq, tok_all), F32),
            jax.ShapeDtypeStruct((tok_all, d), BF16),
            jax.ShapeDtypeStruct((1, tb), F32),
            jax.ShapeDtypeStruct((1, tb), F32),
        ],
        input_output_aliases={} if first else {4: 0, 5: 1},
        compiler_params=params(),
        cost_estimate=pl.CostEstimate(flops=2 * vq * tb * d, bytes_accessed=2 * vq * d + 4 * vq * tb, transcendentals=vq * tb),
        name="logits",
    )(stage, fa, fb, e_bf, *(() if first else prev))


def grad_body(unit, k_width, lg_ref, f_ref, m_ref, w_ref, lab_ref, g_ref, t, t_width):
    rows = lg_ref.shape[0]
    base = pl.program_id(0) * rows
    for k in range(t_width // k_width):
        cols = slice(k * k_width, (k + 1) * k_width)
        row = lax.broadcasted_iota(jnp.int32, (rows, k_width), 0)
        prob = jnp.exp(lg_ref[:, cols] - m_ref[:, cols]) * w_ref[:, cols]
        dl = (prob - jnp.where(row == lab_ref[:, cols] - base, unit, 0.0)).astype(BF16)
        toks = pl.ds(pl.multiple_of(t * t_width + k * k_width, k_width), k_width)
        g_ref[...] += jnp.dot(dl, f_ref[toks, :], preferred_element_type=F32)


def grad_local_kernel(unit, k_width, lg_ref, f_ref, m_ref, w_ref, lab_ref, g_ref):
    t = pl.program_id(1)

    @pl.when(t == 0)
    def _():
        g_ref[...] = jnp.zeros_like(g_ref)

    grad_body(unit, k_width, lg_ref, f_ref, m_ref, w_ref, lab_ref, g_ref, t, lg_ref.shape[1])


def grad_remote_kernel(unit, k_width, n_pre, off_ref, lg_ref, f_ref, m_ref, w_ref, lab_ref, gin_ref, key_ref, srt_ref, g_ref, sq_ref, buf, sem):
    v, t = pl.program_id(0), pl.program_id(1)
    rows, chunk = g_ref.shape[0], buf.shape[1]
    c_lo = off_ref[v] // chunk
    c_hi = (off_ref[v + 1] + chunk - 1) // chunk
    c_hi = jnp.where(off_ref[v + 1] > off_ref[v], c_hi, c_lo)

    def fetch(c, slot):
        return pltpu.make_async_copy(srt_ref.at[pl.ds(pl.multiple_of(c * chunk, chunk), chunk), :], buf.at[slot], sem.at[slot])

    def add_rows(c, slot):
        row = lax.broadcasted_iota(jnp.int32, (rows, chunk), 0)
        hot = jnp.where(row == key_ref[c] - v * rows, 1.0, 0.0).astype(BF16)
        g_ref[...] += jnp.dot(hot, buf[slot], preferred_element_type=F32)

    @pl.when(t == 0)
    def _():
        g_ref[...] = gin_ref[...]
        for j in range(n_pre):
            @pl.when(c_lo + j < c_hi)
            def _():
                fetch(c_lo + j, j).start()

    grad_body(unit, k_width, lg_ref, f_ref, m_ref, w_ref, lab_ref, g_ref, t, lg_ref.shape[1])

    @pl.when(t == pl.num_programs(1) - 1)
    def _():
        for j in range(n_pre):
            @pl.when(c_lo + j < c_hi)
            def _():
                fetch(c_lo + j, j).wait()
                add_rows(c_lo + j, j)

        @pl.loop(c_lo + n_pre, c_hi)
        def _(c):
            fetch(c, 0).start()
            fetch(c, 0).wait()
            add_rows(c, 0)

        @pl.when(v == 0)
        def _():
            sq_ref[...] = jnp.zeros_like(sq_ref)

        sq_ref[...] += jnp.sum(g_ref[...] * g_ref[...], axis=0, keepdims=True)


def grad_call(lg, f_bf, peak, weight, lab, unit, half, vb, tb, k_width, extra=None):
    vq, tok_all = lg.shape
    tok, d = tok_all // 2, f_bf.shape[1]
    n_t = tok // tb
    rest = (lambda f: f) if extra is None else (lambda f: (lambda v, t, *_: f(v, t)))
    in_specs = [
        pl.BlockSpec((vb, tb), rest(lambda v, t: (v, half * n_t + t))),
        pl.BlockSpec((tok, d), rest(lambda v, t: (half, 0)), pipeline_mode=pl.Buffered(1)),
        pl.BlockSpec((1, tb), rest(lambda v, t: (0, t))),
        pl.BlockSpec((1, tb), rest(lambda v, t: (0, t))),
        pl.BlockSpec((1, tb), rest(lambda v, t: (0, t))),
    ]
    g_spec = pl.BlockSpec((vb, d), rest(lambda v, t: (v, 0)))
    g_shape = jax.ShapeDtypeStruct((vq, d), F32)
    cost = pl.CostEstimate(flops=2 * vq * tok * d, bytes_accessed=4 * vq * (tok + 2 * d), transcendentals=vq * tok)
    if extra is None:
        return pl.pallas_call(
            functools.partial(grad_local_kernel, unit, k_width),
            grid=(vq // vb, n_t),
            in_specs=in_specs,
            out_specs=g_spec,
            out_shape=g_shape,
            compiler_params=params(2),
            cost_estimate=cost,
            name="grad_local",
        )(lg, f_bf, peak, weight, lab)
    offs, g_in, keys, srt, chunk = extra
    n_pre = 4
    return pl.pallas_call(
        functools.partial(grad_remote_kernel, unit, k_width, n_pre),
        grid_spec=pltpu.PrefetchScalarGridSpec(
            num_scalar_prefetch=1,
            grid=(vq // vb, n_t),
            in_specs=in_specs + [g_spec, pl.BlockSpec(keys.shape, lambda v, t, *_: (0, 0, 0)), pl.BlockSpec(memory_space=ANY)],
            out_specs=[g_spec, pl.BlockSpec((1, d), lambda v, t, *_: (0, 0))],
            scratch_shapes=[pltpu.VMEM((n_pre, chunk, d), BF16), pltpu.SemaphoreType.DMA((n_pre,))],
        ),
        out_shape=[g_shape, jax.ShapeDtypeStruct((1, d), F32)],
        input_output_aliases={6: 0},
        compiler_params=params(2),
        cost_estimate=cost,
        name="grad_remote",
    )(offs, lg, f_bf, peak, weight, lab, g_in, keys, srt)


def gather_kernel(chunk, bounds, info_ref, order_ref, *refs):
    n_src = len(bounds)
    src_a, src_b, out_ref, buf, sem = refs[:n_src], refs[n_src : 2 * n_src], refs[-3], refs[-2], refs[-1]
    c = pl.program_id(0)
    n_own = info_ref[0]

    def issue(srcs):
        slot = lax.rem(c, 2)

        @pl.loop(0, chunk)
        def _(j):
            tok = order_ref[c * chunk + j]

            def start(q):
                row = tok - (bounds[q - 1] if q else 0)
                pltpu.make_async_copy(srcs[q].at[pl.ds(row, 1), :], buf.at[slot, pl.ds(j, 1), :], sem.at[slot]).start()

            def tree(lo, hi):
                if hi - lo == 1:
                    start(lo)
                    return
                mid = (lo + hi) // 2
                pl.when(tok < bounds[mid - 1])(lambda: tree(lo, mid))
                pl.when(tok >= bounds[mid - 1])(lambda: tree(mid, hi))

            tree(0, n_src)

    @pl.when(c * chunk < n_own)
    def _():
        pl.when(info_ref[1] == 0)(lambda: issue(src_a))
        pl.when(info_ref[1] == 1)(lambda: issue(src_b))

    @pl.when(jnp.logical_and(c >= 1, (c - 1) * chunk < n_own))
    def _():
        slot = lax.rem(c + 1, 2)
        pltpu.make_async_copy(buf.at[slot], buf.at[slot], sem.at[slot]).wait()
        out_ref[...] = buf[slot].astype(BF16)


def gather_call(info, order, srcs_a, srcs_b, chunk):
    d = srcs_a[0].shape[1]
    bounds, total = [], 0
    for src in srcs_a:
        total += src.shape[0]
        bounds.append(total)
    n_chunk = total // chunk

    def out_map(c, info_ref, order_ref):
        last = jnp.maximum((info_ref[0] + chunk - 1) // chunk - 1, 0)
        return (jnp.minimum(jnp.maximum(c - 1, 0), last), 0)

    return pl.pallas_call(
        functools.partial(gather_kernel, chunk, bounds),
        grid_spec=pltpu.PrefetchScalarGridSpec(
            num_scalar_prefetch=2,
            grid=(n_chunk + 1,),
            in_specs=[pl.BlockSpec(memory_space=ANY)] * (2 * len(srcs_a)),
            out_specs=pl.BlockSpec((chunk, d), out_map),
            scratch_shapes=[pltpu.VMEM((2, chunk, d), F32), pltpu.SemaphoreType.DMA((2,))],
        ),
        out_shape=jax.ShapeDtypeStruct((total, d), BF16),
        compiler_params=params(),
        cost_estimate=pl.CostEstimate(flops=30_000_000_000, bytes_accessed=total * d * 4, transcendentals=0),
        name="gather_rows",
    )(info, order, *srcs_a, *srcs_b)


def adamw_kernel(off_ref, scale_ref, e_ref, m_ref, v_ref, g_ref, *rest):
    ne_ref, nm_ref, nv_ref, nb_ref = rest[-4:]
    grad = g_ref[...] * scale_ref[0]
    new_avg = BETA_ONE * m_ref[...] + (1.0 - BETA_ONE) * grad
    new_sq = BETA_TWO * v_ref[...] + (1.0 - BETA_TWO) * grad * grad
    step_dir = (new_avg / (1.0 - BETA_ONE**OPT_STEP)) / (jnp.sqrt(new_sq / (1.0 - BETA_TWO**OPT_STEP)) + ADAM_EPS)
    master = e_ref[...]
    new_master = master - LEARN_RATE * (step_dir + WEIGHT_DECAY * master)
    ne_ref[...] = new_master
    nm_ref[...] = new_avg
    nv_ref[...] = new_sq
    nb_ref[...] = new_master.astype(BF16)


def adamw_call(off, scale, master, exp_avg, exp_avg_sq, grad, vb, prev):
    rows, d = grad.shape
    first = prev is None
    here = pl.BlockSpec((vb, d), lambda i, off_ref, sc: (off_ref[0] + i, 0))
    shape = jax.ShapeDtypeStruct(master.shape, F32)
    return pl.pallas_call(
        adamw_kernel,
        grid_spec=pltpu.PrefetchScalarGridSpec(
            num_scalar_prefetch=2,
            grid=(rows // vb,),
            in_specs=[here, here, here, pl.BlockSpec((vb, d), lambda i, off_ref, sc: (i, 0))]
            + ([] if first else [pl.BlockSpec(memory_space=ANY)] * 4),
            out_specs=[here] * 4,
        ),
        out_shape=[shape, shape, shape, jax.ShapeDtypeStruct(master.shape, BF16)],
        input_output_aliases={} if first else {6: 0, 7: 1, 8: 2, 9: 3},
        compiler_params=params(),
        cost_estimate=pl.CostEstimate(flops=80_000_000_000, bytes_accessed=rows * d * 30, transcendentals=0),
        name="adamw",
    )(off, scale, master, exp_avg, exp_avg_sq, grad, *(() if first else prev))


def permute(x, flip, stage=None, to_other_core=False):
    pairs = []
    for t in range(2):
        for r in range(2):
            for s in range(2):
                if stage is not None and s != stage:
                    continue
                dst = (t ^ ("tp" in flip), r ^ ("dp" in flip), s ^ ("pp" in flip))
                pairs.append((4 * t + 2 * r + s, 4 * dst[0] + 2 * dst[1] + dst[2]))
    return lax.ppermute(x, AXES, pairs)


def after(x, *deps):
    return lax.optimization_barrier((x,) + deps)[0]


def merge_stats(m_a, z_a, m_b, z_b):
    peak = jnp.maximum(m_a, m_b)
    return peak, z_a * jnp.exp(m_a - peak) + z_b * jnp.exp(m_b - peak)


def swap_halves(x):
    half = x.shape[1] // 2
    return jnp.concatenate([x[:, half:], x[:, :half]], axis=1)


def reduce_stats(m, z, far):
    for axis in ("pp", "tp"):
        other = permute(jnp.concatenate([m, z], axis=0), axis)
        if far and axis == "tp":
            other = swap_halves(other)
        m, z = merge_stats(m, z, other[0:1], other[1:2])
    return m, z


def solution(mesh):
    assert all(mesh.shape[a] == 2 for a in AXES)
    table_spec = P("tp", None)

    def device_step(master, exp_avg, exp_avg_sq, stage_ids, stage_acts):
        tp, dp, pp = (lax.axis_index(a) for a in AXES)
        v_dev, d = master.shape
        vq = v_dev // 2
        tok = stage_ids.shape[1] * stage_ids.shape[2]
        half = tok // 2
        tb = tok // 6
        n_half = half // tb
        vb1, vb2, vb3 = vq // 5, vq // 10, vq // 20
        chunk = 256
        stage = pp.astype(jnp.int32).reshape(1)
        act = stage_acts.reshape(tok, d)
        ids = stage_ids.reshape(1, tok)

        def part(start, size):
            return lax.dynamic_slice(act, (start, 0), (size, d)).astype(F32)

        own = [act[:tb].astype(F32), act[tb:].astype(F32)]
        own = list(lax.optimization_barrier(tuple(own)))
        send = [lax.optimization_barrier(part(tp * half + k * tb, tb)) for k in range(n_half)]
        sib = [permute(x, "pp") for x in own]
        sib_ids = permute(ids, "pp")

        fx = [permute(x, "dp", 1) for x in send]
        fy = [permute(x, "tp", 1) for x in fx]
        fxs = [permute(x, "pp", 1) for x in fx]
        fys = [permute(x, "pp", 1) for x in fy]

        tok_ids = jnp.where(pp == 0, ids, sib_ids)
        labels = jnp.where(pp == 0, sib_ids, ids)
        both = jnp.concatenate([tok_ids, labels], axis=0)
        far = permute(both, "dp")
        far = jnp.where(tp == 0, far, swap_halves(far))
        all_ids = jnp.concatenate([both, far], axis=1) - (2 * tp + pp) * vq

        key = all_ids[0]
        mine = jnp.logical_and(key >= 0, key < vq)
        key = jnp.where(mine, key, vq)
        keys, order = lax.sort((key, lax.iota(jnp.int32, 2 * tok)), num_keys=1, is_stable=False)
        edges = jnp.arange(vq // vb2 + 1, dtype=jnp.int32) * vb2
        offs = jnp.sum((key[None, :] < edges[:, None]).astype(jnp.int32), axis=1)
        info = jnp.stack([offs[-1], pp.astype(jnp.int32)])

        e_bf = lax.dynamic_slice(master, (pp * vq, 0), (vq, d)).astype(BF16)

        prev, stats = None, []
        for c in range(4 * n_half):
            if c < 2 * n_half:
                fb, fb_blk = (sib[0], 0) if c == 0 else (sib[1], c - 1)
                fa, fa_blk = act, c
            else:
                k = c - 2 * n_half
                fa, fb = (fx[k], fxs[k]) if k < n_half else (fy[k - n_half], fys[k - n_half])
                fa_blk = fb_blk = 0
            lg, f_bf, m, z = logits_call(stage, fa, fa_blk, fb, fb_blk, e_bf, c, tb, vb1, 2 * tok, prev)
            prev = (lg, f_bf)
            stats.append((m, z))

        n_dx, dxb = 2, half // 2
        dx = [after(part(tp * half + k * dxb, dxb), fxs[-1]) for k in range(n_dx)]
        dx = [permute(x, "dp", 0) for x in dx]
        dy = [permute(x, "tp", 0) for x in dx]
        dxs = [permute(x, "pp", 0) for x in dx]
        dys = [permute(x, "pp", 0) for x in dy]

        def joined(parts, far):
            return reduce_stats(*(jnp.concatenate([p[i] for p in parts], axis=1) for i in range(2)), far)

        m_loc, z_loc = joined(stats[: 2 * n_half], False)
        unit = 1.0 / tok
        g_loc = grad_call(lg, f_bf, m_loc, unit / z_loc, all_ids[1:2, :tok], unit, 0, vb2, tok // 2, tb)
        m_far, z_far = joined(stats[2 * n_half :], True)
        srt = gather_call(info, order, own + dx + dy, sib + dxs + dys, chunk)
        extra = (offs, g_loc, keys.reshape(-1, 1, chunk), srt, chunk)
        grad, sq = grad_call(lg, f_bf, m_far, unit / z_far, all_ids[1:2, tok:], unit, 1, vb2, tok // 2, tb, extra)

        other = permute(grad, "pp")
        sq_total = lax.psum(jnp.sum(sq), ("tp", "pp")) * 0.25
        scale = (0.5 * (CLIP_NORM / jnp.maximum(jnp.sqrt(sq_total), CLIP_NORM))).reshape(1)
        n_blk = vq // vb3
        outs = adamw_call(stage * n_blk, scale, master, exp_avg, exp_avg_sq, grad, vb3, None)
        return tuple(adamw_call((1 - stage) * n_blk, scale, master, exp_avg, exp_avg_sq, other, vb3, outs))

    return jax.shard_map(
        device_step,
        mesh=mesh,
        in_specs=(table_spec, table_spec, table_spec, P("pp", "dp", None), P("pp", "dp", None, None)),
        out_specs=(table_spec, table_spec, table_spec, table_spec),
        check_vma=False,
    )
```

```python
import functools

import jax
import jax.numpy as jnp
from jax import lax
from jax.experimental import pallas as pl
from jax.experimental.pallas import tpu as pltpu
from jax.sharding import PartitionSpec as P


LEARN_RATE = 0.003
BETA_ONE = 0.9
BETA_TWO = 0.95
ADAM_EPS = 1e-8
WEIGHT_DECAY = 0.1
CLIP_NORM = 1.0
OPT_STEP = 10
VMEM_CAP = 63 * 1024 * 1024
F32 = jnp.float32
BF16 = jnp.bfloat16
AXES = ("tp", "dp", "pp")
ANY = pl.ANY


def params(n_axes=1):
    return pltpu.CompilerParams(dimension_semantics=("arbitrary",) * n_axes, vmem_limit_bytes=VMEM_CAP)


def logits_kernel(n_sub, starts, stage_ref, *refs):
    n_src = len(starts)
    fa_refs, fb_refs, e_ref = refs[:n_src], refs[n_src : 2 * n_src], refs[2 * n_src]
    lg_ref, f_ref, m_ref, z_ref = refs[-4:]
    t = pl.program_id(0)

    @pl.when(pl.program_id(1) == 0)
    def _():
        for j in range(n_src):
            here = t >= starts[j]
            if j + 1 < n_src:
                here = jnp.logical_and(here, t < starts[j + 1])

            @pl.when(jnp.logical_and(here, stage_ref[0] == 1))
            def _(j=j):
                f_ref[...] = fa_refs[j][...].astype(BF16)

            @pl.when(jnp.logical_and(here, stage_ref[0] == 0))
            def _(j=j):
                f_ref[...] = fb_refs[j][...].astype(BF16)

        m_ref[...] = jnp.full_like(m_ref, -jnp.inf)
        z_ref[...] = jnp.zeros_like(z_ref)

    width = f_ref.shape[0] // n_sub
    for j in range(n_sub):
        cols = slice(j * width, (j + 1) * width)
        lg_ref[:, cols] = lax.dot_general(e_ref[...], f_ref[cols, :], (((1,), (1,)), ((), ())), preferred_element_type=F32)
        m_old = m_ref[:, cols]
        m_new = jnp.maximum(m_old, jnp.max(lg_ref[:, cols], axis=0, keepdims=True))
        part = jnp.sum(jnp.exp(lg_ref[:, cols] - m_new), axis=0, keepdims=True)
        z_ref[:, cols] = z_ref[:, cols] * jnp.exp(m_old - m_new) + part
        m_ref[:, cols] = m_new


def logits_call(stage, srcs, e_bf, t_blk, tb, vb, tok, prev):
    vq, d = e_bf.shape
    first = prev is None
    starts, n_t = [], 0
    for src in srcs:
        starts.append(n_t)
        n_t += src[4]

    def src_spec(blk, start, count):
        mode = {"pipeline_mode": pl.Buffered(1)} if count == 1 else {}
        return pl.BlockSpec((tb, d), lambda t, v, s: (blk + jnp.clip(t - start, 0, count - 1), 0), **mode)

    in_specs = [src_spec(src[1], st, src[4]) for src, st in zip(srcs, starts)]
    in_specs += [src_spec(src[3], st, src[4]) for src, st in zip(srcs, starts)]
    in_specs += [pl.BlockSpec((vb, d), lambda t, v, s: (v, 0))]
    in_specs += [] if first else [pl.BlockSpec(memory_space=ANY)] * 2
    out_specs = [
        pl.BlockSpec((vb, tb), lambda t, v, s: (v, t_blk + t)),
        pl.BlockSpec((tb, d), lambda t, v, s: (t_blk + t, 0)),
        pl.BlockSpec((1, tb), lambda t, v, s: (0, t)),
        pl.BlockSpec((1, tb), lambda t, v, s: (0, t)),
    ]
    n_sub = max(1, tb // 256)
    n_in = 2 * len(srcs) + 2
    return pl.pallas_call(
        functools.partial(logits_kernel, n_sub, starts),
        grid_spec=pltpu.PrefetchScalarGridSpec(num_scalar_prefetch=1, grid=(n_t, vq // vb), in_specs=in_specs, out_specs=out_specs),
        out_shape=[
            jax.ShapeDtypeStruct((vq, tok), F32),
            jax.ShapeDtypeStruct((tok, d), BF16),
            jax.ShapeDtypeStruct((1, n_t * tb), F32),
            jax.ShapeDtypeStruct((1, n_t * tb), F32),
        ],
        input_output_aliases={} if first else {n_in: 0, n_in + 1: 1},
        compiler_params=params(2),
        cost_estimate=pl.CostEstimate(
            flops=2 * vq * n_t * tb * d, bytes_accessed=n_t * (2 * vq * d + 4 * vq * tb), transcendentals=vq * n_t * tb
        ),
        name="logits",
    )(stage, *[src[0] for src in srcs], *[src[2] for src in srcs], e_bf, *(() if first else prev))


def grad_body(unit, k_width, lg_ref, f_ref, m_ref, w_ref, lab_ref, g_ref, t, t_width):
    rows = lg_ref.shape[0]
    base = pl.program_id(0) * rows
    for k in range(t_width // k_width):
        cols = slice(k * k_width, (k + 1) * k_width)
        row = lax.broadcasted_iota(jnp.int32, (rows, k_width), 0)
        prob = jnp.exp(lg_ref[:, cols] - m_ref[:, cols]) * w_ref[:, cols]
        dl = (prob - jnp.where(row == lab_ref[:, cols] - base, unit, 0.0)).astype(BF16)
        toks = pl.ds(pl.multiple_of(t * t_width + k * k_width, k_width), k_width)
        g_ref[...] += jnp.dot(dl, f_ref[toks, :], preferred_element_type=F32)


def grad_local_kernel(unit, k_width, lg_ref, f_ref, m_ref, w_ref, lab_ref, g_ref):
    t = pl.program_id(1)

    @pl.when(t == 0)
    def _():
        g_ref[...] = jnp.zeros_like(g_ref)

    grad_body(unit, k_width, lg_ref, f_ref, m_ref, w_ref, lab_ref, g_ref, t, lg_ref.shape[1])


def grad_remote_kernel(unit, k_width, n_pre, off_ref, lg_ref, f_ref, m_ref, w_ref, lab_ref, gin_ref, key_ref, srt_ref, g_ref, sq_ref, buf, sem):
    v, t = pl.program_id(0), pl.program_id(1)
    rows, chunk = g_ref.shape[0], buf.shape[2]
    c_lo = off_ref[v] // chunk
    c_hi = (off_ref[v + 1] + chunk - 1) // chunk
    c_hi = jnp.where(off_ref[v + 1] > off_ref[v], c_hi, c_lo)

    def fetch(c, slot):
        return pltpu.make_async_copy(srt_ref.at[:, pl.ds(pl.multiple_of(c * chunk, chunk), chunk), :], buf.at[slot], sem.at[slot])

    def add_rows(c, slot):
        row = lax.broadcasted_iota(jnp.int32, (rows, chunk), 0)
        hot = jnp.where(row == key_ref[c] - v * rows, 1.0, 0.0).astype(BF16)
        for i in range(3):
            g_ref[...] += jnp.dot(hot, buf[slot, i], preferred_element_type=F32)

    @pl.when(t == 0)
    def _():
        g_ref[...] = gin_ref[...]
        for j in range(n_pre):
            @pl.when(c_lo + j < c_hi)
            def _():
                fetch(c_lo + j, j).start()

    grad_body(unit, k_width, lg_ref, f_ref, m_ref, w_ref, lab_ref, g_ref, t, lg_ref.shape[1])

    @pl.when(t == pl.num_programs(1) - 1)
    def _():
        for j in range(n_pre):
            @pl.when(c_lo + j < c_hi)
            def _():
                fetch(c_lo + j, j).wait()
                add_rows(c_lo + j, j)

        @pl.loop(c_lo + n_pre, c_hi)
        def _(c):
            fetch(c, 0).start()
            fetch(c, 0).wait()
            add_rows(c, 0)

        @pl.when(v == 0)
        def _():
            sq_ref[...] = jnp.zeros_like(sq_ref)

        sq_ref[...] += jnp.sum(g_ref[...] * g_ref[...], axis=0, keepdims=True)


def grad_call(lg, f_bf, peak, weight, lab, unit, vb, tb, k_width, extra=None):
    vq, tok = lg.shape
    d = f_bf.shape[1]
    n_t = tok // tb
    rest = (lambda f: f) if extra is None else (lambda f: (lambda v, t, *_: f(v, t)))
    in_specs = [
        pl.BlockSpec((vb, tb), rest(lambda v, t: (v, t))),
        pl.BlockSpec((tok, d), rest(lambda v, t: (0, 0)), pipeline_mode=pl.Buffered(1)),
        pl.BlockSpec((1, tb), rest(lambda v, t: (0, t))),
        pl.BlockSpec((1, tb), rest(lambda v, t: (0, t))),
        pl.BlockSpec((1, tb), rest(lambda v, t: (0, t))),
    ]
    g_spec = pl.BlockSpec((vb, d), rest(lambda v, t: (v, 0)))
    g_shape = jax.ShapeDtypeStruct((vq, d), F32)
    cost = pl.CostEstimate(flops=2 * vq * tok * d, bytes_accessed=4 * vq * (tok + 2 * d), transcendentals=vq * tok)
    if extra is None:
        return pl.pallas_call(
            functools.partial(grad_local_kernel, unit, k_width),
            grid=(vq // vb, n_t),
            in_specs=in_specs,
            out_specs=g_spec,
            out_shape=g_shape,
            compiler_params=params(2),
            cost_estimate=cost,
            name="grad_local",
        )(lg, f_bf, peak, weight, lab)
    offs, g_in, keys, srt, chunk = extra
    n_pre = 3
    return pl.pallas_call(
        functools.partial(grad_remote_kernel, unit, k_width, n_pre),
        grid_spec=pltpu.PrefetchScalarGridSpec(
            num_scalar_prefetch=1,
            grid=(vq // vb, n_t),
            in_specs=in_specs + [g_spec, pl.BlockSpec(keys.shape, lambda v, t, *_: (0, 0, 0)), pl.BlockSpec(memory_space=ANY)],
            out_specs=[g_spec, pl.BlockSpec((1, d), lambda v, t, *_: (0, 0))],
            scratch_shapes=[pltpu.VMEM((n_pre, 3, chunk, d), BF16), pltpu.SemaphoreType.DMA((n_pre,))],
        ),
        out_shape=[g_shape, jax.ShapeDtypeStruct((1, d), F32)],
        input_output_aliases={6: 0},
        compiler_params=params(2),
        cost_estimate=cost,
        name="grad_remote",
    )(offs, lg, f_bf, peak, weight, lab, g_in, keys, srt)


def distinct_kernel(n_stage_rows, blocks, info_ref, uk_ref, key_ref, *refs):
    n_src = (len(refs) - 4) // 2
    src_a, src_b = refs[:n_src], refs[n_src : 2 * n_src]
    out_ref, dx_ref, buf, sem = refs[-4:]
    c = pl.program_id(0)
    chunk = out_ref.shape[1]
    depth = buf.shape[0]

    @pl.when(c == 0)
    def _():
        def start(i):
            q, row = blocks[i]

            @pl.when(info_ref[1] == 0)
            def _():
                pltpu.make_async_copy(src_a[q].at[pl.ds(row, n_stage_rows), :], buf.at[i % depth], sem.at[i % depth]).start()

            @pl.when(info_ref[1] == 1)
            def _():
                pltpu.make_async_copy(src_b[q].at[pl.ds(row, n_stage_rows), :], buf.at[i % depth], sem.at[i % depth]).start()

        for i in range(min(depth - 1, len(blocks))):
            start(i)
        for i in range(len(blocks)):
            if i + depth - 1 < len(blocks):
                start(i + depth - 1)
            pltpu.make_async_copy(src_a[0].at[pl.ds(0, n_stage_rows), :], buf.at[i % depth], sem.at[i % depth]).wait()
            dx_ref[i * n_stage_rows : (i + 1) * n_stage_rows, :] = buf[i % depth].astype(BF16)

    @pl.when(c < info_ref[0])
    def _():
        n_tok = dx_ref.shape[0]
        width = n_tok // 6
        acc = jnp.zeros((chunk, dx_ref.shape[1]), F32)
        for k in range(6):
            cols = slice(k * width, (k + 1) * width)
            hot = jnp.where(uk_ref[...] == key_ref[:, cols], 1.0, 0.0).astype(BF16)
            acc += jnp.dot(hot, dx_ref[cols, :], preferred_element_type=F32)
        high = acc.astype(BF16)
        rest = acc - high.astype(F32)
        mid = rest.astype(BF16)
        out_ref[0] = high
        out_ref[1] = mid
        out_ref[2] = (rest - mid.astype(F32)).astype(BF16)


def distinct_call(info, uk, key, srcs_a, srcs_b, chunk, n_stage_rows):
    d = srcs_a[0].shape[1]
    blocks = [(q, row) for q, src in enumerate(srcs_a) for row in range(0, src.shape[0], n_stage_rows)]
    cap = uk.shape[0]
    n_tok = key.shape[1]

    def last(c, info_ref):
        return jnp.minimum(c, jnp.maximum(info_ref[0] - 1, 0))

    return pl.pallas_call(
        functools.partial(distinct_kernel, n_stage_rows, blocks),
        grid_spec=pltpu.PrefetchScalarGridSpec(
            num_scalar_prefetch=1,
            grid=(cap // chunk,),
            in_specs=[pl.BlockSpec((chunk, 1), lambda c, i: (last(c, i), 0)), pl.BlockSpec((1, n_tok), lambda c, i: (0, 0))]
            + [pl.BlockSpec(memory_space=ANY)] * (2 * len(srcs_a)),
            out_specs=pl.BlockSpec((3, chunk, d), lambda c, i: (0, last(c, i), 0)),
            scratch_shapes=[pltpu.VMEM((n_tok, d), BF16), pltpu.VMEM((4, n_stage_rows, d), F32), pltpu.SemaphoreType.DMA((4,))],
        ),
        out_shape=jax.ShapeDtypeStruct((3, cap, d), BF16),
        compiler_params=params(),
        cost_estimate=pl.CostEstimate(flops=40_000_000_000, bytes_accessed=n_tok * d * 4, transcendentals=0),
        name="distinct_sums",
    )(info, uk, key, *srcs_a, *srcs_b)


def adamw_kernel(off_ref, scale_ref, e_ref, m_ref, v_ref, g_ref, *rest):
    ne_ref, nm_ref, nv_ref, nb_ref = rest[-4:]
    grad = g_ref[...] * scale_ref[0]
    new_avg = BETA_ONE * m_ref[...] + (1.0 - BETA_ONE) * grad
    new_sq = BETA_TWO * v_ref[...] + (1.0 - BETA_TWO) * grad * grad
    step_dir = (new_avg / (1.0 - BETA_ONE**OPT_STEP)) / (jnp.sqrt(new_sq / (1.0 - BETA_TWO**OPT_STEP)) + ADAM_EPS)
    master = e_ref[...]
    new_master = master - LEARN_RATE * (step_dir + WEIGHT_DECAY * master)
    ne_ref[...] = new_master
    nm_ref[...] = new_avg
    nv_ref[...] = new_sq
    nb_ref[...] = new_master.astype(BF16)


def adamw_call(off, scale, master, exp_avg, exp_avg_sq, grad, vb, prev):
    rows, d = grad.shape
    first = prev is None
    here = pl.BlockSpec((vb, d), lambda i, off_ref, sc: (off_ref[0] + i, 0))
    shape = jax.ShapeDtypeStruct(master.shape, F32)
    return pl.pallas_call(
        adamw_kernel,
        grid_spec=pltpu.PrefetchScalarGridSpec(
            num_scalar_prefetch=2,
            grid=(rows // vb,),
            in_specs=[here, here, here, pl.BlockSpec((vb, d), lambda i, off_ref, sc: (i, 0))]
            + ([] if first else [pl.BlockSpec(memory_space=ANY)] * 4),
            out_specs=[here] * 4,
        ),
        out_shape=[shape, shape, shape, jax.ShapeDtypeStruct(master.shape, BF16)],
        input_output_aliases={} if first else {6: 0, 7: 1, 8: 2, 9: 3},
        compiler_params=params(),
        cost_estimate=pl.CostEstimate(flops=80_000_000_000, bytes_accessed=rows * d * 30, transcendentals=0),
        name="adamw",
    )(off, scale, master, exp_avg, exp_avg_sq, grad, *(() if first else prev))


def permute(x, flip, stage=None):
    pairs = []
    for t in range(2):
        for r in range(2):
            for s in range(2):
                if stage is not None and s != stage:
                    continue
                dst = (t ^ ("tp" in flip), r ^ ("dp" in flip), s ^ ("pp" in flip))
                pairs.append((4 * t + 2 * r + s, 4 * dst[0] + 2 * dst[1] + dst[2]))
    return lax.ppermute(x, AXES, pairs)


def after(x, *deps):
    return lax.optimization_barrier((x,) + deps)[0]


def swap_halves(x):
    half = x.shape[1] // 2
    return jnp.concatenate([x[:, half:], x[:, :half]], axis=1)


def reduce_stats(m, z, far, then):
    mine = jnp.concatenate([m, z], axis=0)
    others = [permute(mine, flip) for flip in ("pp", "tp", "tp pp")]
    others = [after(x, then) for x in others]
    if far:
        others[1:] = [swap_halves(x) for x in others[1:]]
    peak = m
    for x in others:
        peak = jnp.maximum(peak, x[0:1])
    total = z * jnp.exp(m - peak)
    for x in others:
        total = total + x[1:2] * jnp.exp(x[0:1] - peak)
    return peak, total


def solution(mesh):
    assert all(mesh.shape[a] == 2 for a in AXES)
    table_spec = P("tp", None)

    def stage_step(master, exp_avg, exp_avg_sq, stage_ids, stage_acts):
        tp, _, pp = (lax.axis_index(a) for a in AXES)
        v_dev, d = master.shape
        vq = v_dev // 2
        tok = stage_ids.shape[1] * stage_ids.shape[2]
        half = tok // 2
        tb = tok // 6
        dxb = half // 2
        vb1, vb2, vb3 = vq // 5, vq // 10, vq // 20
        chunk = 256
        stage = pp.astype(jnp.int32).reshape(1)
        act = stage_acts.reshape(tok, d)
        ids = stage_ids.reshape(1, tok)

        def part(source, start, size):
            return lax.dynamic_slice(source, (start, 0), (size, d)).astype(F32)

        zero = lax.optimization_barrier(jnp.int32(0))
        fx = [lax.optimization_barrier(part(act, tp * half, 2 * tb))]
        fx.append(lax.optimization_barrier(part(after(act, fx[0]), tp * half + 2 * tb, tb)))
        own = [lax.optimization_barrier(part(after(act, fx[0], fx[1]), zero, tb))]
        own.append(lax.optimization_barrier(part(after(act, own[0]), zero + tb, tok - tb)))
        e_bf = lax.dynamic_slice(after(master, own[1]), (pp * vq, 0), (vq, d)).astype(BF16)
        sib = [permute(own[0], "pp"), permute(own[1], "pp")]
        fx = [permute(fx[0], "dp", 1), permute(fx[1], "dp", 1)]

        lg_a = logits_call(stage, [(act, 0, sib[0], 0, 1)], e_bf, 0, tb, vb1, tok, None)
        lg_b = logits_call(stage, [(act, 1, sib[1], 0, 2)], e_bf, 1, tb, vb1, tok, lg_a[:2])
        fx0 = after(fx[0], lg_b[2])
        fy0, fxs0 = permute(fx0, "tp", 1), permute(fx0, "pp", 1)
        act_b = after(act, lg_b[2])
        dx = [permute(lax.optimization_barrier(part(act_b, tp * half + k * dxb, dxb)), "dp", 0) for k in range(2)]
        lg_c = logits_call(stage, [(act, 3, sib[1], 2, 3)], e_bf, 3, tb, vb1, tok, lg_b[:2])
        fx1 = after(fx[1], lg_c[2])
        fy1, fxs1 = permute(fx1, "tp", 1), permute(fx1, "pp", 1)

        sib_ids, far_ids, far_sib = (permute(ids, flip) for flip in ("pp", "dp", "dp pp"))
        sib_ids, far_ids, far_sib = (after(x, lg_c[2]) for x in (sib_ids, far_ids, far_sib))
        near = jnp.concatenate([jnp.where(pp == 0, ids, sib_ids), jnp.where(pp == 0, sib_ids, ids)], axis=0)
        far = jnp.concatenate([jnp.where(pp == 0, far_ids, far_sib), jnp.where(pp == 0, far_sib, far_ids)], axis=0)
        far = jnp.where(tp == 0, far, swap_halves(far))
        all_ids = jnp.concatenate([near, far], axis=1) - (2 * tp + pp) * vq

        key = all_ids[0]
        key = jnp.where(jnp.logical_and(key >= 0, key < vq), key, vq)
        srt = lax.sort(key)
        new = jnp.concatenate([srt[:1] < vq, jnp.logical_and(srt[1:] != srt[:-1], srt[1:] < vq)])
        cap = min(-(-vq // chunk) * chunk, 2 * tok)
        uk = lax.sort(jnp.where(new, srt, 2 * vq))[:cap]
        edges = jnp.arange(vq // vb2 + 1, dtype=jnp.int32) * vb2
        offs = jnp.sum((uk[None, :] < edges[:, None]).astype(jnp.int32), axis=1)
        info = jnp.stack([(offs[-1] + chunk - 1) // chunk, pp.astype(jnp.int32)])

        src = [(after(fx[0], lg_c[2]), 0, after(fxs0, lg_c[2]), 0, 2)]
        fr_a = logits_call(stage, src, e_bf, 0, tb, vb1, tok, None)
        m_loc, z_loc = reduce_stats(*(jnp.concatenate([lg_a[i], lg_b[i], lg_c[i]], axis=1) for i in (2, 3)), False, fr_a[2])
        fys0, fys1 = permute(after(fy0, fr_a[2]), "pp", 1), permute(after(fy1, fr_a[2]), "pp", 1)
        dx0 = after(dx[0], fr_a[2])
        dy0, dxs0 = permute(dx0, "tp", 0), permute(dx0, "pp", 0)
        unit = 1.0 / tok
        lg_loc = after(lg_c[0], fr_a[2])
        g_loc = grad_call(lg_loc, lg_c[1], m_loc, unit / z_loc, all_ids[1:2, :tok], unit, vb2, tok // 2, tb)
        dx1 = after(dx[1], g_loc)
        dy1, dxs1 = permute(dx1, "tp", 0), permute(dx1, "pp", 0)
        dys0 = permute(after(dy0, g_loc), "pp", 0)
        e_far = after(e_bf, g_loc)
        rest = [(after(fx1, g_loc), 0, after(fxs1, g_loc), 0, 1), (after(fy0, g_loc), 0, after(fys0, g_loc), 0, 2)]
        rest.append((after(fy1, g_loc), 0, after(fys1, g_loc), 0, 1))
        fr_b = logits_call(stage, rest, e_far, 2, tb, vb1, tok, fr_a[:2])
        dys1 = permute(after(dy1, fr_b[2]), "pp", 0)
        srcs = own + [dx[0], dx[1], dy0, dy1], sib + [after(dxs0, fr_b[2]), after(dxs1, fr_b[2]), after(dys0, fr_b[2]), dys1]
        sums = distinct_call(info, uk.reshape(-1, 1), key.reshape(1, -1), *srcs, chunk, tb // 2)
        m_far, z_far = reduce_stats(*(jnp.concatenate([fr_a[i], fr_b[i]], axis=1) for i in (2, 3)), True, sums)
        extra = (offs, g_loc, uk.reshape(-1, 1, chunk), sums, chunk)
        grad, sq = grad_call(fr_b[0], fr_b[1], m_far, unit / z_far, all_ids[1:2, tok:], unit, vb2, tok // 2, tb, extra)

        other = permute(grad, "pp")
        sq_total = lax.psum(jnp.sum(sq), ("tp", "pp")) * 0.25
        scale = (0.5 * (CLIP_NORM / jnp.maximum(jnp.sqrt(sq_total), CLIP_NORM))).reshape(1)
        n_blk = vq // vb3
        outs = adamw_call(stage * n_blk, scale, master, exp_avg, exp_avg_sq, grad, vb3, None)
        return tuple(adamw_call((1 - stage) * n_blk, scale, master, exp_avg, exp_avg_sq, other, vb3, outs))

    return jax.shard_map(
        stage_step,
        mesh=mesh,
        in_specs=(table_spec, table_spec, table_spec, P("pp", "dp", None), P("pp", "dp", None, None)),
        out_specs=(table_spec, table_spec, table_spec, table_spec),
        check_vma=False,
    )
```

```python
import functools

import jax
import jax.numpy as jnp
from jax import lax
from jax.experimental import pallas as pl
from jax.experimental.pallas import tpu as pltpu
from jax.sharding import PartitionSpec as P


LEARN_RATE = 0.003
BETA_ONE = 0.9
BETA_TWO = 0.95
ADAM_EPS = 1e-8
WEIGHT_DECAY = 0.1
CLIP_NORM = 1.0
OPT_STEP = 10
VMEM_CAP = 67043328
F32 = jnp.float32
BF16 = jnp.bfloat16
AXES = ("tp", "dp", "pp")
ANY = pl.ANY


def params(n_axes=1):
    return pltpu.CompilerParams(dimension_semantics=("arbitrary",) * n_axes, vmem_limit_bytes=VMEM_CAP)


def logits_kernel(n_sub, starts, stage_ref, *refs):
    n_src = len(starts)
    fa_refs, fb_refs, e_ref = refs[:n_src], refs[n_src : 2 * n_src], refs[2 * n_src]
    lg_ref, f_ref, m_ref, z_ref = refs[-4:]
    t = pl.program_id(0)

    @pl.when(pl.program_id(1) == 0)
    def _():
        for j in range(n_src):
            here = t >= starts[j]
            if j + 1 < n_src:
                here = jnp.logical_and(here, t < starts[j + 1])

            @pl.when(jnp.logical_and(here, stage_ref[0] == 1))
            def _(j=j):
                f_ref[...] = fa_refs[j][...].astype(BF16)

            @pl.when(jnp.logical_and(here, stage_ref[0] == 0))
            def _(j=j):
                f_ref[...] = fb_refs[j][...].astype(BF16)

        m_ref[...] = jnp.full_like(m_ref, -jnp.inf)
        z_ref[...] = jnp.zeros_like(z_ref)

    width = f_ref.shape[0] // n_sub
    for j in range(n_sub):
        cols = slice(j * width, (j + 1) * width)
        lg_ref[:, cols] = lax.dot_general(e_ref[...], f_ref[cols, :], (((1,), (1,)), ((), ())), preferred_element_type=F32)
        m_old = m_ref[:, cols]
        m_new = jnp.maximum(m_old, jnp.max(lg_ref[:, cols], axis=0, keepdims=True))
        part = jnp.sum(jnp.exp(lg_ref[:, cols] - m_new), axis=0, keepdims=True)
        z_ref[:, cols] = z_ref[:, cols] * jnp.exp(m_old - m_new) + part
        m_ref[:, cols] = m_new


def logits_call(stage, srcs, e_bf, t_blk, tb, vb, tok, prev):
    vq, d = e_bf.shape
    first = prev is None
    starts, n_t = [], 0
    for src in srcs:
        starts.append(n_t)
        n_t += src[4]

    def src_spec(blk, start, count):
        mode = {"pipeline_mode": pl.Buffered(1)} if count == 1 else {}
        return pl.BlockSpec((tb, d), lambda t, v, s: (blk + jnp.clip(t - start, 0, count - 1), 0), **mode)

    in_specs = [src_spec(src[1], st, src[4]) for src, st in zip(srcs, starts)]
    in_specs += [src_spec(src[3], st, src[4]) for src, st in zip(srcs, starts)]
    in_specs += [pl.BlockSpec((vb, d), lambda t, v, s: (v, 0))]
    in_specs += [] if first else [pl.BlockSpec(memory_space=ANY)] * 2
    out_specs = [
        pl.BlockSpec((vb, tb), lambda t, v, s: (v, t_blk + t)),
        pl.BlockSpec((tb, d), lambda t, v, s: (t_blk + t, 0)),
        pl.BlockSpec((1, tb), lambda t, v, s: (0, t)),
        pl.BlockSpec((1, tb), lambda t, v, s: (0, t)),
    ]
    n_sub = max(1, tb // 256)
    n_in = 2 * len(srcs) + 2
    return pl.pallas_call(
        functools.partial(logits_kernel, n_sub, starts),
        grid_spec=pltpu.PrefetchScalarGridSpec(num_scalar_prefetch=1, grid=(n_t, vq // vb), in_specs=in_specs, out_specs=out_specs),
        out_shape=[
            jax.ShapeDtypeStruct((vq, tok), F32),
            jax.ShapeDtypeStruct((tok, d), BF16),
            jax.ShapeDtypeStruct((1, n_t * tb), F32),
            jax.ShapeDtypeStruct((1, n_t * tb), F32),
        ],
        input_output_aliases={} if first else {n_in: 0, n_in + 1: 1},
        compiler_params=params(2),
        cost_estimate=pl.CostEstimate(
            flops=2 * vq * n_t * tb * d, bytes_accessed=n_t * (2 * vq * d + 4 * vq * tb), transcendentals=vq * n_t * tb
        ),
        name="logits",
    )(stage, *[src[0] for src in srcs], *[src[2] for src in srcs], e_bf, *(() if first else prev))


def grad_body(unit, k_width, lg_ref, f_ref, m_ref, w_ref, lab_ref, g_ref, t, t_width):
    rows = lg_ref.shape[0]
    base = pl.program_id(0) * rows
    for k in range(t_width // k_width):
        cols = slice(k * k_width, (k + 1) * k_width)
        row = lax.broadcasted_iota(jnp.int32, (rows, k_width), 0)
        prob = jnp.exp(lg_ref[:, cols] - m_ref[:, cols]) * w_ref[:, cols]
        dl = (prob - jnp.where(row == lab_ref[:, cols] - base, unit, 0.0)).astype(BF16)
        toks = pl.ds(pl.multiple_of(t * t_width + k * k_width, k_width), k_width)
        g_ref[...] += jnp.dot(dl, f_ref[toks, :], preferred_element_type=F32)


def grad_local_kernel(unit, k_width, lg_ref, f_ref, m_ref, w_ref, lab_ref, g_ref):
    t = pl.program_id(1)

    @pl.when(t == 0)
    def _():
        g_ref[...] = jnp.zeros_like(g_ref)

    grad_body(unit, k_width, lg_ref, f_ref, m_ref, w_ref, lab_ref, g_ref, t, lg_ref.shape[1])


def grad_remote_kernel(unit, k_width, n_pre, off_ref, lg_ref, f_ref, m_ref, w_ref, lab_ref, gin_ref, key_ref, srt_ref, g_ref, sq_ref, buf, sem):
    v, t = pl.program_id(0), pl.program_id(1)
    rows, chunk = g_ref.shape[0], buf.shape[2]
    c_lo = off_ref[v] // chunk
    c_hi = (off_ref[v + 1] + chunk - 1) // chunk
    c_hi = jnp.where(off_ref[v + 1] > off_ref[v], c_hi, c_lo)

    def fetch(c, slot):
        return pltpu.make_async_copy(srt_ref.at[:, pl.ds(pl.multiple_of(c * chunk, chunk), chunk), :], buf.at[slot], sem.at[slot])

    def add_rows(c, slot):
        row = lax.broadcasted_iota(jnp.int32, (rows, chunk), 0)
        hot = jnp.where(row == key_ref[c] - v * rows, 1.0, 0.0).astype(BF16)
        for i in range(3):
            g_ref[...] += jnp.dot(hot, buf[slot, i], preferred_element_type=F32)

    @pl.when(t == 0)
    def _():
        g_ref[...] = gin_ref[...]
        for j in range(n_pre):
            @pl.when(c_lo + j < c_hi)
            def _():
                fetch(c_lo + j, j).start()

    grad_body(unit, k_width, lg_ref, f_ref, m_ref, w_ref, lab_ref, g_ref, t, lg_ref.shape[1])

    @pl.when(t == pl.num_programs(1) - 1)
    def _():
        for j in range(n_pre):
            @pl.when(c_lo + j < c_hi)
            def _():
                fetch(c_lo + j, j).wait()
                add_rows(c_lo + j, j)

        @pl.loop(c_lo + n_pre, c_hi)
        def _(c):
            fetch(c, 0).start()
            fetch(c, 0).wait()
            add_rows(c, 0)

        @pl.when(v == 0)
        def _():
            sq_ref[...] = jnp.zeros_like(sq_ref)

        sq_ref[...] += jnp.sum(g_ref[...] * g_ref[...], axis=0, keepdims=True)


def grad_call(lg, f_bf, peak, weight, lab, unit, vb, tb, k_width, extra=None):
    vq, tok = lg.shape
    d = f_bf.shape[1]
    n_t = tok // tb
    rest = (lambda f: f) if extra is None else (lambda f: (lambda v, t, *_: f(v, t)))
    in_specs = [
        pl.BlockSpec((vb, tb), rest(lambda v, t: (v, t))),
        pl.BlockSpec((tok, d), rest(lambda v, t: (0, 0)), pipeline_mode=pl.Buffered(1)),
        pl.BlockSpec((1, tb), rest(lambda v, t: (0, t))),
        pl.BlockSpec((1, tb), rest(lambda v, t: (0, t))),
        pl.BlockSpec((1, tb), rest(lambda v, t: (0, t))),
    ]
    g_spec = pl.BlockSpec((vb, d), rest(lambda v, t: (v, 0)))
    g_shape = jax.ShapeDtypeStruct((vq, d), F32)
    cost = pl.CostEstimate(flops=2 * vq * tok * d, bytes_accessed=4 * vq * (tok + 2 * d), transcendentals=vq * tok)
    if extra is None:
        return pl.pallas_call(
            functools.partial(grad_local_kernel, unit, k_width),
            grid=(vq // vb, n_t),
            in_specs=in_specs,
            out_specs=g_spec,
            out_shape=g_shape,
            compiler_params=params(2),
            cost_estimate=cost,
            name="grad_local",
        )(lg, f_bf, peak, weight, lab)
    offs, g_in, keys, srt, chunk = extra
    n_pre = 2
    return pl.pallas_call(
        functools.partial(grad_remote_kernel, unit, k_width, n_pre),
        grid_spec=pltpu.PrefetchScalarGridSpec(
            num_scalar_prefetch=1,
            grid=(vq // vb, n_t),
            in_specs=in_specs + [g_spec, pl.BlockSpec(keys.shape, lambda v, t, *_: (0, 0, 0)), pl.BlockSpec(memory_space=ANY)],
            out_specs=[g_spec, pl.BlockSpec((1, d), lambda v, t, *_: (0, 0))],
            scratch_shapes=[pltpu.VMEM((n_pre, 3, chunk, d), BF16), pltpu.SemaphoreType.DMA((n_pre,))],
        ),
        out_shape=[g_shape, jax.ShapeDtypeStruct((1, d), F32)],
        input_output_aliases={6: 0},
        compiler_params=params(2),
        cost_estimate=cost,
        name="grad_remote",
    )(offs, lg, f_bf, peak, weight, lab, g_in, keys, srt)


def distinct_kernel(n_stage_rows, blocks, info_ref, uk_ref, key_ref, *refs):
    n_src = (len(refs) - 4) // 2
    src_a, src_b = refs[:n_src], refs[n_src : 2 * n_src]
    out_ref, dx_ref, buf, sem = refs[-4:]
    c = pl.program_id(0)
    chunk = out_ref.shape[1]
    depth = buf.shape[0]

    @pl.when(c == 0)
    def _():
        def start(i):
            q, row = blocks[i]

            @pl.when(info_ref[1] == 0)
            def _():
                pltpu.make_async_copy(src_a[q].at[pl.ds(row, n_stage_rows), :], buf.at[i % depth], sem.at[i % depth]).start()

            @pl.when(info_ref[1] == 1)
            def _():
                pltpu.make_async_copy(src_b[q].at[pl.ds(row, n_stage_rows), :], buf.at[i % depth], sem.at[i % depth]).start()

        for i in range(min(depth - 1, len(blocks))):
            start(i)
        for i in range(len(blocks)):
            if i + depth - 1 < len(blocks):
                start(i + depth - 1)
            pltpu.make_async_copy(src_a[0].at[pl.ds(0, n_stage_rows), :], buf.at[i % depth], sem.at[i % depth]).wait()
            dx_ref[i * n_stage_rows : (i + 1) * n_stage_rows, :] = buf[i % depth].astype(BF16)

    @pl.when(c < info_ref[0])
    def _():
        n_tok = dx_ref.shape[0]
        width = n_tok // 6
        acc = jnp.zeros((chunk, dx_ref.shape[1]), F32)
        for k in range(6):
            cols = slice(k * width, (k + 1) * width)
            hot = jnp.where(uk_ref[...] == key_ref[:, cols], 1.0, 0.0).astype(BF16)
            acc += jnp.dot(hot, dx_ref[cols, :], preferred_element_type=F32)
        high = acc.astype(BF16)
        rest = acc - high.astype(F32)
        mid = rest.astype(BF16)
        out_ref[0] = high
        out_ref[1] = mid
        out_ref[2] = (rest - mid.astype(F32)).astype(BF16)


def distinct_call(info, uk, key, srcs_a, srcs_b, chunk, n_stage_rows):
    d = srcs_a[0].shape[1]
    blocks = [(q, row) for q, src in enumerate(srcs_a) for row in range(0, src.shape[0], n_stage_rows)]
    cap = uk.shape[0]
    n_tok = key.shape[1]

    def last(c, info_ref):
        return jnp.minimum(c, jnp.maximum(info_ref[0] - 1, 0))

    return pl.pallas_call(
        functools.partial(distinct_kernel, n_stage_rows, blocks),
        grid_spec=pltpu.PrefetchScalarGridSpec(
            num_scalar_prefetch=1,
            grid=(cap // chunk,),
            in_specs=[pl.BlockSpec((chunk, 1), lambda c, i: (last(c, i), 0)), pl.BlockSpec((1, n_tok), lambda c, i: (0, 0))]
            + [pl.BlockSpec(memory_space=ANY)] * (2 * len(srcs_a)),
            out_specs=pl.BlockSpec((3, chunk, d), lambda c, i: (0, last(c, i), 0)),
            scratch_shapes=[pltpu.VMEM((n_tok, d), BF16), pltpu.VMEM((4, n_stage_rows, d), F32), pltpu.SemaphoreType.DMA((4,))],
        ),
        out_shape=jax.ShapeDtypeStruct((3, cap, d), BF16),
        compiler_params=params(),
        cost_estimate=pl.CostEstimate(flops=40_000_000_000, bytes_accessed=n_tok * d * 4, transcendentals=0),
        name="distinct_sums",
    )(info, uk, key, *srcs_a, *srcs_b)


def adamw_kernel(off_ref, scale_ref, e_ref, m_ref, v_ref, g_ref, *rest):
    ne_ref, nm_ref, nv_ref, nb_ref = rest[-4:]
    grad = g_ref[...] * scale_ref[0]
    new_avg = BETA_ONE * m_ref[...] + (1.0 - BETA_ONE) * grad
    new_sq = BETA_TWO * v_ref[...] + (1.0 - BETA_TWO) * grad * grad
    step_dir = (new_avg / (1.0 - BETA_ONE**OPT_STEP)) / (jnp.sqrt(new_sq / (1.0 - BETA_TWO**OPT_STEP)) + ADAM_EPS)
    master = e_ref[...]
    new_master = master - LEARN_RATE * (step_dir + WEIGHT_DECAY * master)
    ne_ref[...] = new_master
    nm_ref[...] = new_avg
    nv_ref[...] = new_sq
    nb_ref[...] = new_master.astype(BF16)


def adamw_call(off, scale, master, exp_avg, exp_avg_sq, grad, vb, prev):
    rows, d = grad.shape
    first = prev is None
    here = pl.BlockSpec((vb, d), lambda i, off_ref, sc: (off_ref[0] + i, 0))
    shape = jax.ShapeDtypeStruct(master.shape, F32)
    return pl.pallas_call(
        adamw_kernel,
        grid_spec=pltpu.PrefetchScalarGridSpec(
            num_scalar_prefetch=2,
            grid=(rows // vb,),
            in_specs=[here, here, here, pl.BlockSpec((vb, d), lambda i, off_ref, sc: (i, 0))]
            + ([] if first else [pl.BlockSpec(memory_space=ANY)] * 4),
            out_specs=[here] * 4,
        ),
        out_shape=[shape, shape, shape, jax.ShapeDtypeStruct(master.shape, BF16)],
        input_output_aliases={} if first else {6: 0, 7: 1, 8: 2, 9: 3},
        compiler_params=params(),
        cost_estimate=pl.CostEstimate(flops=80_000_000_000, bytes_accessed=rows * d * 30, transcendentals=0),
        name="adamw",
    )(off, scale, master, exp_avg, exp_avg_sq, grad, *(() if first else prev))


def permute(x, flip, stage=None):
    pairs = []
    for t in range(2):
        for r in range(2):
            for s in range(2):
                if stage is not None and s != stage:
                    continue
                dst = (t ^ ("tp" in flip), r ^ ("dp" in flip), s ^ ("pp" in flip))
                pairs.append((4 * t + 2 * r + s, 4 * dst[0] + 2 * dst[1] + dst[2]))
    return lax.ppermute(x, AXES, pairs)


def after(x, *deps):
    return lax.optimization_barrier((x,) + deps)[0]


def swap_halves(x):
    half = x.shape[1] // 2
    return jnp.concatenate([x[:, half:], x[:, :half]], axis=1)


def reduce_stats(m, z, far, then):
    mine = jnp.concatenate([m, z], axis=0)
    others = [permute(mine, flip) for flip in ("pp", "tp", "tp pp")]
    others = [after(x, then) for x in others]
    if far:
        others[1:] = [swap_halves(x) for x in others[1:]]
    peak = m
    for x in others:
        peak = jnp.maximum(peak, x[0:1])
    total = z * jnp.exp(m - peak)
    for x in others:
        total = total + x[1:2] * jnp.exp(x[0:1] - peak)
    return peak, total


def solution(mesh):
    assert all(mesh.shape[a] == 2 for a in AXES)
    table_spec = P("tp", None)

    def stage_step(master, exp_avg, exp_avg_sq, stage_ids, stage_acts):
        tp, _, pp = (lax.axis_index(a) for a in AXES)
        v_dev, d = master.shape
        vq = v_dev // 2
        tok = stage_ids.shape[1] * stage_ids.shape[2]
        half = tok // 2
        tb = tok // 6
        dxb = half // 2
        vb1, vb2, vb3 = vq // 4, vq // 10, vq // 20
        chunk = 256
        stage = pp.astype(jnp.int32).reshape(1)
        act = stage_acts.reshape(tok, d)
        ids = stage_ids.reshape(1, tok)

        def part(source, start, size):
            return lax.dynamic_slice(source, (start, 0), (size, d)).astype(F32)

        zero = lax.optimization_barrier(jnp.int32(0))
        fx = [lax.optimization_barrier(part(act, tp * half, 2 * tb))]
        fx.append(lax.optimization_barrier(part(after(act, fx[0]), tp * half + 2 * tb, tb)))
        own = [lax.optimization_barrier(part(after(act, fx[0], fx[1]), zero, tb))]
        own.append(lax.optimization_barrier(part(after(act, own[0]), zero + tb, tok - tb)))
        e_bf = lax.dynamic_slice(after(master, own[1]), (pp * vq, 0), (vq, d)).astype(BF16)
        sib = [permute(own[0], "pp"), permute(own[1], "pp")]
        fx = [permute(fx[0], "dp", 1), permute(fx[1], "dp", 1)]

        lg_a = logits_call(stage, [(act, 0, sib[0], 0, 1)], e_bf, 0, tb, vb1, tok, None)
        lg_b = logits_call(stage, [(act, 1, sib[1], 0, 2)], e_bf, 1, tb, vb1, tok, lg_a[:2])
        fx0 = after(fx[0], lg_b[2])
        fy0, fxs0 = permute(fx0, "tp", 1), permute(fx0, "pp", 1)
        act_b = after(act, lg_b[2])
        dx = [permute(lax.optimization_barrier(part(act_b, tp * half + k * dxb, dxb)), "dp", 0) for k in range(2)]
        lg_c = logits_call(stage, [(act, 3, sib[1], 2, 3)], e_bf, 3, tb, vb1, tok, lg_b[:2])
        fx1 = after(fx[1], lg_c[2])
        fy1, fxs1 = permute(fx1, "tp", 1), permute(fx1, "pp", 1)

        sib_ids, far_ids, far_sib = (permute(ids, flip) for flip in ("pp", "dp", "dp pp"))
        sib_ids, far_ids, far_sib = (after(x, lg_c[2]) for x in (sib_ids, far_ids, far_sib))
        near = jnp.concatenate([jnp.where(pp == 0, ids, sib_ids), jnp.where(pp == 0, sib_ids, ids)], axis=0)
        far = jnp.concatenate([jnp.where(pp == 0, far_ids, far_sib), jnp.where(pp == 0, far_sib, far_ids)], axis=0)
        far = jnp.where(tp == 0, far, swap_halves(far))
        all_ids = jnp.concatenate([near, far], axis=1) - (2 * tp + pp) * vq

        key = all_ids[0]
        key = jnp.where(jnp.logical_and(key >= 0, key < vq), key, vq)
        srt = lax.sort(key)
        new = jnp.concatenate([srt[:1] < vq, jnp.logical_and(srt[1:] != srt[:-1], srt[1:] < vq)])
        cap = min(-(-vq // chunk) * chunk, 2 * tok)
        uk = lax.sort(jnp.where(new, srt, 2 * vq))[:cap]
        edges = jnp.arange(vq // vb2 + 1, dtype=jnp.int32) * vb2
        offs = jnp.sum((uk[None, :] < edges[:, None]).astype(jnp.int32), axis=1)
        info = jnp.stack([(offs[-1] + chunk - 1) // chunk, pp.astype(jnp.int32)])

        src = [(after(fx[0], lg_c[2]), 0, after(fxs0, lg_c[2]), 0, 2)]
        fr_a = logits_call(stage, src, e_bf, 0, tb, vb1, tok, None)
        m_loc, z_loc = reduce_stats(*(jnp.concatenate([lg_a[i], lg_b[i], lg_c[i]], axis=1) for i in (2, 3)), False, fr_a[2])
        fys0, fys1 = permute(after(fy0, fr_a[2]), "pp", 1), permute(after(fy1, fr_a[2]), "pp", 1)
        dx0 = after(dx[0], fr_a[2])
        dy0, dxs0 = permute(dx0, "tp", 0), permute(dx0, "pp", 0)
        unit = 1.0 / tok
        lg_loc = after(lg_c[0], fr_a[2])
        g_loc = grad_call(lg_loc, lg_c[1], m_loc, unit / z_loc, all_ids[1:2, :tok], unit, vb2, tok, tb)
        dx1 = after(dx[1], g_loc)
        dy1, dxs1 = permute(dx1, "tp", 0), permute(dx1, "pp", 0)
        dys0 = permute(after(dy0, g_loc), "pp", 0)
        e_far = after(e_bf, g_loc)
        rest = [(after(fx1, g_loc), 0, after(fxs1, g_loc), 0, 1), (after(fy0, g_loc), 0, after(fys0, g_loc), 0, 2)]
        rest.append((after(fy1, g_loc), 0, after(fys1, g_loc), 0, 1))
        fr_b = logits_call(stage, rest, e_far, 2, tb, vb1, tok, fr_a[:2])
        dys1 = permute(after(dy1, fr_b[2]), "pp", 0)
        srcs = own + [dx[0], dx[1], dy0, dy1], sib + [after(dxs0, fr_b[2]), after(dxs1, fr_b[2]), after(dys0, fr_b[2]), dys1]
        sums = distinct_call(info, uk.reshape(-1, 1), key.reshape(1, -1), *srcs, chunk, tb // 2)
        m_far, z_far = reduce_stats(*(jnp.concatenate([fr_a[i], fr_b[i]], axis=1) for i in (2, 3)), True, sums)
        extra = (offs, g_loc, uk.reshape(-1, 1, chunk), sums, chunk)
        grad, sq = grad_call(fr_b[0], fr_b[1], m_far, unit / z_far, all_ids[1:2, tok:], unit, vb2, tok, tb, extra)

        sq_total = lax.psum(jnp.sum(sq), ("tp", "pp")) * 0.25
        scale = (0.5 * (CLIP_NORM / jnp.maximum(jnp.sqrt(sq_total), CLIP_NORM))).reshape(1)
        other = permute(after(grad, scale), "pp")
        n_blk = vq // vb3
        outs = adamw_call(stage * n_blk, scale, master, exp_avg, exp_avg_sq, grad, vb3, None)
        return tuple(adamw_call((1 - stage) * n_blk, scale, master, exp_avg, exp_avg_sq, other, vb3, outs))

    return jax.shard_map(
        stage_step,
        mesh=mesh,
        in_specs=(table_spec, table_spec, table_spec, P("pp", "dp", None), P("pp", "dp", None, None)),
        out_specs=(table_spec, table_spec, table_spec, table_spec),
        check_vma=False,
    )
```
